32 devices in a mesh: leaf: 8 (over z, y), grp: 4 (over x, core).
Axes of the slice: x: 2, y: 2, z: 4, core: 2. Of those that a mesh axis runs over, the one named last changes fastest.
Arguments:
- points: bfloat16 [32768, 256], P(('leaf', 'grp')), may hold values from -0.75 to 0.75
- rhs: float32 [32768, 128], P(('leaf', 'grp')), may hold values from -0.8 to 0.8
- permutation: int32 [32768], P(('leaf', 'grp')), may hold values from 0 to 32767, as said below
- leaf_basis: float32 [8192, 1024], P(('leaf', 'grp')), may hold values from -0.1875 to 0.1875
- climb_leaf: float32 [8192, 256], P(('leaf', 'grp')), may hold values from -0.25 to 0.25
- climb_pair: float32 [4096, 256], P(('leaf', 'grp')), may hold values from -0.25 to 0.25
- climb_quad: float32 [2048, 256], P(('leaf', 'grp')), may hold values from -0.25 to 0.25
- skel_points: bfloat16 [1024, 256], P(('leaf', 'grp')), may hold values from -0.75 to 0.75
- near_lists: int32 [32, 8], replicated, may hold values from -1 to 31, as said below
- far_lists: int32 [4, 3], replicated, may hold values from -1 to 3, as said below
Outputs:
- product: float32 [32768, 128], P(('leaf', 'grp'))
The draws below stay inside these ranges and needn't reach their ends.
Inputs may be any that keep to these rules, and one draw needn't show every extreme that they name: `permutation`: maps each block of 1024 tree positions of one leaf onto the same block of initial indices, each once. `near_lists`: row t starts with t itself, then distinct other leaves of the same aligned block of eight (t // 8), then -1 entries only; some row has 8 leaves. `far_lists`: row m holds one or more distinct nodes other than m first, then -1 entries only; some row has 3 nodes.
All inputs are finite; a program needn't handle non-finite values.
Results may differ from the reference program's by a relative error of at most 0.0003.
Values may be sent and summed in bfloat16 or wider, within the bound.
No kernel may reach another device: no remote copies, remote signals or barrier semaphores. Data moves between devices by JAX's collectives and lax.ppermute only.
A program may use at most 128 MiB of HBM per device.

```python
import jax
import jax.numpy as jnp
from jax import lax

D = 256
S = 256
LEAF_SIZE = 1024
NEARMAX = 8
NRHS = 128
LEAVES = 32
POINTS = 32768
NODES = 4
FARMAX = 3


def shared_frame(key):
    return jax.random.normal(jax.random.fold_in(key, 101), (8, D), jnp.float32) / jnp.sqrt(jnp.float32(D))


def point_cloud(key, rows, group, salt):
    frame = shared_frame(key)
    keys = jax.random.split(jax.random.fold_in(key, salt), 4)
    groups = rows // group
    centre = jax.random.normal(keys[0], (groups, 8), jnp.float32)
    spread = jax.random.normal(keys[1], (rows, 8), jnp.float32)
    low_scale = jnp.log(jnp.float32(0.6))
    high_scale = jnp.log(jnp.float32(1.6))
    latent = 0.7 * jnp.repeat(centre, group, axis=0) + spread
    latent = latent / jnp.sqrt(jnp.float32(8 * 1.49))
    direction = jnp.dot(latent, frame)
    noise = jax.random.normal(keys[2], (rows, D), jnp.float32) * (0.5 / jnp.sqrt(jnp.float32(D)))
    scales = jnp.exp(jax.random.uniform(keys[3], (rows, 1), jnp.float32, low_scale, high_scale))
    values = jnp.clip(scales * (direction + noise), -0.75, 0.75)
    return values.astype(jnp.bfloat16)


def draw_points(key, part):
    return point_cloud(key, POINTS, LEAF_SIZE, 31)


def draw_skel_points(key, part):
    return point_cloud(key, NODES * S, S, 37)


def draw_permutation(key, part):
    base = jax.random.fold_in(key, 7)

    def one_leaf(leaf):
        order = jax.random.permutation(jax.random.fold_in(base, leaf), jnp.arange(LEAF_SIZE, dtype=jnp.int32))
        return order + leaf * LEAF_SIZE
    blocks = jax.vmap(one_leaf)(jnp.arange(LEAVES, dtype=jnp.int32))
    return blocks.reshape(POINTS).astype(jnp.int32)


def draw_near_lists(key, part):
    first, second, third = jax.random.split(jax.random.fold_in(key, 11), 3)
    leaf_ids = jnp.arange(LEAVES, dtype=jnp.int32)
    pick = jax.random.randint(first, (LEAVES,), 0, 8)
    count = jnp.where(pick < 4, 1, jnp.where(pick < 7, 2, 3))
    busiest = jax.random.randint(second, (), 0, LEAVES)
    count = jnp.where(leaf_ids == busiest, NEARMAX, count)
    scores = jax.random.randint(third, (LEAVES, 8), 0, 2 ** 20) * 8 + jnp.arange(8, dtype=jnp.int32)[None, :]
    mine = (leaf_ids % 8)[:, None] == jnp.arange(8, dtype=jnp.int32)[None, :]
    scores = jnp.where(mine, -1, scores)
    order = jnp.argsort(scores, axis=1, stable=True).astype(jnp.int32)
    candidates = (leaf_ids // 8)[:, None] * 8 + order
    slots = jnp.arange(NEARMAX, dtype=jnp.int32)
    return jnp.where(slots[None, :] < count[:, None], candidates[:, :NEARMAX], -1).astype(jnp.int32)


def draw_far_lists(key, part):
    first, second, third, fourth = jax.random.split(jax.random.fold_in(key, 23), 4)
    node_ids = jnp.arange(NODES, dtype=jnp.int32)
    popular = jax.random.randint(first, (NODES,), 0, 4)
    noise = jax.random.randint(second, (NODES, NODES), 0, 2 ** 20)
    scores = popular[None, :] * 2 ** 20 + noise
    scores = jnp.where(node_ids[:, None] == node_ids[None, :], -1, scores)
    order = jnp.argsort(-scores, axis=1, stable=True).astype(jnp.int32)
    pick = jax.random.randint(third, (NODES,), 0, 4)
    count = jnp.minimum(1 + 2 * pick, FARMAX)
    busiest = jax.random.randint(fourth, (), 0, NODES)
    count = jnp.where(node_ids == busiest, FARMAX, count)
    slots = jnp.arange(FARMAX, dtype=jnp.int32)
    return jnp.where(slots[None, :] < count[:, None], order[:, :FARMAX], -1).astype(jnp.int32)


def shard_levels(stream_key, shape, cuts, smallest, top_value):
    level = 1.0
    for dim, blocks in cuts:
        heights = jax.random.uniform(jax.random.fold_in(jax.random.fold_in(stream_key, 6), dim), (blocks,), jnp.float32, smallest / len(cuts), top_value / len(cuts))
        level = level * jnp.repeat(jnp.exp(heights), shape[dim] // blocks).reshape((-1,) + (1,) * (len(shape) - 1 - dim))
    return level


def bell_draw(rng, extent, deviation, limit, pieces=(), kind=jnp.bfloat16):
    factor_of = shard_levels(rng, extent, pieces, -0.22, 0.18) if pieces else 1.0
    drawn = jax.random.normal(rng, extent, jnp.float32) * deviation * factor_of
    return jnp.minimum(jnp.maximum(drawn, -limit), limit).astype(kind)


def setup_inputs(seed: int = 0) -> dict:
    seeds = jax.random.split(jax.random.key(seed), 11)
    points = draw_points(jax.random.fold_in(seeds[10], 71), 0)
    rhs = bell_draw(seeds[1], (POINTS, NRHS), 0.1, 0.8, ((0, 32),), jnp.float32)
    permutation = draw_permutation(jax.random.fold_in(seeds[10], 71), 0)
    leaf_basis = bell_draw(seeds[3], (LEAVES * S, LEAF_SIZE), LEAF_SIZE ** -0.5, 0.1875, ((0, 32),), jnp.float32)
    climb_leaf = bell_draw(seeds[4], (LEAVES * S, S), (2 * S) ** -0.5, 0.25, ((0, 32),), jnp.float32)
    climb_pair = bell_draw(seeds[5], (LEAVES // 2 * S, S), (2 * S) ** -0.5, 0.25, ((0, 32),), jnp.float32)
    climb_quad = bell_draw(seeds[6], (LEAVES // 4 * S, S), (2 * S) ** -0.5, 0.25, ((0, 32),), jnp.float32)
    skel_points = draw_skel_points(jax.random.fold_in(seeds[10], 71), 0)
    near_lists = draw_near_lists(jax.random.fold_in(seeds[10], 71), 0)
    far_lists = draw_far_lists(jax.random.fold_in(seeds[10], 71), 0)
    return dict(points=points, rhs=rhs, permutation=permutation, leaf_basis=leaf_basis, climb_leaf=climb_leaf, climb_pair=climb_pair, climb_quad=climb_quad, skel_points=skel_points, near_lists=near_lists, far_lists=far_lists)


def kernel_block(left, right):
    inner = jnp.dot(left, right.T, preferred_element_type=jnp.float32)
    left_sq = lax.optimization_barrier(jnp.sum(jnp.square(left.astype(jnp.float32)), axis=1))
    right_sq = lax.optimization_barrier(jnp.sum(jnp.square(right.astype(jnp.float32)), axis=1))
    product = left_sq[:, None] * right_sq[None, :]
    sine = jnp.sqrt(jnp.maximum(product - inner * inner, 0.0))
    theta = jnp.arctan2(sine, inner)
    return (sine + (jnp.pi - theta) * inner) / jnp.pi

def reference(points, rhs, permutation, leaf_basis, climb_leaf, climb_pair, climb_quad, skel_points, near_lists, far_lists):
    upper_limit = lax.Precision.HIGHEST
    tree_pts = points[permutation].reshape(LEAVES, LEAF_SIZE, D)
    tree_weight = rhs[permutation].reshape(LEAVES, LEAF_SIZE, NRHS)

    def near_leaf(leaf):
        row = near_lists[leaf]
        count = jnp.sum((row >= 0).astype(jnp.int32))

        def add_block(step, total):
            other = row[step]
            kern = kernel_block(tree_pts[leaf], tree_pts[other])
            return total + jnp.dot(kern, tree_weight[other], precision=upper_limit)
        return lax.fori_loop(0, count, add_block, jnp.zeros((LEAF_SIZE, NRHS), jnp.float32))
    near = lax.map(near_leaf, jnp.arange(LEAVES, dtype=jnp.int32))
    basis_matrix = leaf_basis.reshape(LEAVES, S, LEAF_SIZE)
    block_one = climb_leaf.reshape(LEAVES, S, S)
    block_two = climb_pair.reshape(LEAVES // 2, S, S)
    block_three = climb_quad.reshape(LEAVES // 4, S, S)
    skeleton_level_zero = jnp.einsum('zbg,zgo->zbo', basis_matrix, tree_weight, precision=upper_limit)
    skel_one = jnp.einsum('lab,lan->lbn', block_one, skeleton_level_zero, precision=upper_limit).reshape(LEAVES // 2, 2, S, NRHS).sum(1)
    skel_two = jnp.einsum('lab,lan->lbn', block_two, skel_one, precision=upper_limit).reshape(LEAVES // 4, 2, S, NRHS).sum(1)
    skel_three = jnp.einsum('lab,lan->lbn', block_three, skel_two, precision=upper_limit).reshape(NODES, 2, S, NRHS).sum(1)
    all_weights = skel_three.reshape(NODES * S, NRHS)
    col_node = (jnp.arange(NODES * S) // S).astype(jnp.int32)

    def far_node(node):
        own = lax.dynamic_slice_in_dim(skel_points, node * S, S, 0)
        kern = kernel_block(own, skel_points)
        row = far_lists[node]
        selected_rows = jnp.any(col_node[:, None] == row[None, :], axis=1).astype(jnp.float32)
        return jnp.dot(kern * selected_rows[None, :], all_weights, precision=upper_limit)
    up_three = lax.map(far_node, jnp.arange(NODES, dtype=jnp.int32))
    up_two = jnp.einsum('qab,qbn->qan', block_three, jnp.repeat(up_three, 2, axis=0), precision=upper_limit)
    up_one = jnp.einsum('qab,qbn->qan', block_two, jnp.repeat(up_two, 2, axis=0), precision=upper_limit)
    upward_level_zero = jnp.einsum('qab,qbn->qan', block_one, jnp.repeat(up_one, 2, axis=0), precision=upper_limit)
    distant_field = jnp.einsum('efp,efb->epb', basis_matrix, upward_level_zero, precision=upper_limit)
    total = (near + distant_field).reshape(POINTS, NRHS)
    return jnp.zeros_like(total).at[permutation].set(total)
```

```python
import functools

import jax
import jax.numpy as jnp
from jax import lax
from jax.experimental import pallas as pl
from jax.experimental.pallas import tpu as pltpu
from jax.sharding import PartitionSpec as P

AXES = ("leaf", "grp")
NODE = 8
TINY = 1e-30
SERIES = (
    1.0000000728662903,
    -1.0119652067319684e-05,
    -0.4997682863293359,
    0.2101526158419862,
    -0.11576220091414788,
    0.06085262424317596,
    -0.023177540521381382,
    0.004332679697781438,
)
F32 = jnp.float32
BF16 = jnp.bfloat16
HIGHEST = lax.Precision.HIGHEST
VMEM = pltpu.VMEM
SMEM = pltpu.SMEM


def across(value, mask):
    pairs = [(s, s ^ mask) for s in range(lax.axis_size(AXES))]
    return lax.ppermute(value, AXES, pairs)


def call(kernel, out, n_smem, operands, scratch=(), flops=0, aliases=None):
    specs = [pl.BlockSpec(memory_space=SMEM)] * n_smem
    specs += [pl.BlockSpec(memory_space=VMEM)] * (len(operands) - n_smem)
    multi = isinstance(out, (list, tuple))
    return pl.pallas_call(
        kernel,
        out_shape=out,
        in_specs=specs,
        out_specs=[pl.BlockSpec(memory_space=VMEM)] * len(out)
        if multi
        else pl.BlockSpec(memory_space=VMEM),
        scratch_shapes=list(scratch),
        cost_estimate=pl.CostEstimate(flops=flops, bytes_accessed=0, transcendentals=0),
        compiler_params=pltpu.CompilerParams(vmem_limit_bytes=40 * 2**20),
        input_output_aliases=aliases or {},
    )(*operands)


def halves(value):
    hi = value.astype(BF16)
    return hi, (value - hi.astype(F32)).astype(BF16)


def dot(a, b, dims=((1,), (0,))):
    return lax.dot_general(a, b, (dims, ((), ())), preferred_element_type=F32)


def fine(a, b, dims=((1,), (0,))):
    return lax.dot_general(
        a, b, (dims, ((), ())), precision=HIGHEST, preferred_element_type=F32
    )


def unit_kernel(cosine):
    z = jnp.maximum(1.0 - cosine * cosine, TINY)
    w = z * lax.rsqrt(z)
    acc = jnp.full_like(w, SERIES[-1])
    for coef in SERIES[-2::-1]:
        acc = acc * w + coef
    return acc + cosine


def norms(x):
    x = x.astype(F32)
    sq = jnp.maximum(jnp.sum(x * x, axis=1, keepdims=True), TINY)
    inv = lax.rsqrt(sq)
    return sq * inv, inv


def pack_kernel(x_ref, w_ref, a_ref, b_ref):
    half = x_ref.shape[0] // 2
    width = w_ref.shape[1]
    feats = x_ref.shape[1]
    for k, ref in enumerate((a_ref, b_ref)):
        rows = pl.ds(k * half, half)
        x = x_ref[rows, :]
        ref[0:half, 0:feats] = x
        xf = x.astype(F32)
        length, _ = norms(x)
        hi, lo = halves(w_ref[rows, :] * (length * 0.5))
        ref[0:half, feats : feats + width] = hi
        ref[0:half, feats + width : feats + 2 * width] = lo
        row = fine(jnp.ones((8, feats), F32), xf * xf, ((1,), (1,)))
        inv = lax.rsqrt(jnp.maximum(row, TINY))
        p0 = inv.astype(BF16)
        rest = inv - p0.astype(F32)
        p1 = rest.astype(BF16)
        p2 = (rest - p1.astype(F32)).astype(BF16)
        wide = jnp.zeros((8, ref.shape[1] - half), BF16)
        if wide.shape[1]:
            p0, p1, p2 = (jnp.concatenate([p, wide], 1) for p in (p0, p1, p2))
        ref[half : half + 8, :] = p0
        ref[half + 8 : half + 16, :] = p1
        ref[half + 16 : half + 24, :] = p2
        ref[half + 24 : half + 32, :] = jnp.zeros_like(p0)


def listed(lists_ref, row, value):
    hit = lists_ref[row, 0] == value
    for s in range(1, lists_ref.shape[1]):
        hit = jnp.logical_or(hit, lists_ref[row, s] == value)
    return hit


def near_kernel(masks, first, *refs):
    flat_ref, lists_ref, own_ref, mate_ref = refs[:4]
    packs = refs[4 : 4 + len(masks)]
    sums_in = () if first else refs[4 + len(masks) : 6 + len(masks)]
    outs = refs[-2:]
    flat = flat_ref[0]
    half = own_ref.shape[0] // 2
    feats = own_ref.shape[1]
    width = outs[0].shape[1]
    tile = 256
    steps = own_ref.shape[0] // tile
    for t, (x_ref, out_ref) in enumerate(((own_ref, outs[0]), (mate_ref, outs[1]))):
        if first:
            out_ref[...] = jnp.zeros_like(out_ref)
        else:
            out_ref[...] = sums_in[t][...]
        target = flat ^ t
        for mask, pack in zip(masks, packs):

            @pl.when(listed(lists_ref, target, flat ^ mask))
            def _():
                inv_row = (
                    pack[half : half + 8, 0:half].astype(F32)
                    + pack[half + 8 : half + 16, 0:half].astype(F32)
                    + pack[half + 16 : half + 24, 0:half].astype(F32)
                )[0:1, :]

                def rows(i, carry):
                    at = pl.ds(pl.multiple_of(i * tile, tile), tile)
                    x = x_ref[at, :]
                    length, inv = norms(x)
                    total = jnp.zeros((tile, 2 * width), F32)
                    for j in range(half // 256):
                        src = pl.ds(j * 256, 256)
                        c = dot(x, pack[src, 0:feats], ((1,), (1,)))
                        u = c * inv * inv_row[:, j * 256 : (j + 1) * 256]
                        hi, lo = halves(unit_kernel(u))
                        total = total + dot(hi, pack[src, feats : feats + 2 * width])
                        small = dot(lo, pack[src, feats : feats + width])
                        total = total + jnp.concatenate([small, jnp.zeros_like(small)], 1)
                    out_ref[at, :] += length * (total[:, 0:width] + total[:, width:])
                    return carry

                lax.fori_loop(0, steps, rows, 0)


def basis_kernel(perm_ref, basis_ref, w_ref, first_ref, turned_ref, part_ref, hot_ref):
    size = basis_ref.shape[1]
    rank = basis_ref.shape[0]
    width = w_ref.shape[1]
    place = lax.rem(perm_ref[...], size)
    for i in range(size // 256):
        spot = lax.broadcasted_iota(jnp.int32, (256, size), 0) + i * 256
        hot_ref[i * 256 : (i + 1) * 256, :] = jnp.where(spot == place, 1.0, 0.0).astype(BF16)
    hi, lo = halves(basis_ref[...])
    pair = jnp.concatenate([hi, lo], 0)
    hot = hot_ref[...]
    turned_ref[...] = dot(hot, pair, ((1,), (1,))).astype(BF16)
    moved = dot(pair, hot, ((1,), (1,))).astype(BF16)
    whi, wlo = halves(w_ref[...])
    y = dot(moved, jnp.concatenate([whi, wlo], 1))
    y = y[0:rank, 0:width] + y[0:rank, width:] + y[rank:, 0:width]
    part_ref[...] = fine(first_ref[...], y, ((0,), (0,)))


def climb_kernel(flat_ref, part_ref, own_ref, mate_ref, keep_ref, send_ref, a_ref, b_ref):
    flat = flat_ref[0]
    rank = part_ref.shape[0]
    half, quarter = rank // 2, rank // 4
    parity = flat % 2
    a_ref[...] = part_ref[...]
    total = None
    for k, ref in enumerate((own_ref, mate_ref)):
        at = pl.ds(pl.multiple_of((parity ^ k) * half, half), half)
        term = fine(ref[0:half, :], a_ref[at, :], ((0,), (0,)))
        total = term if total is None else total + term
    b_ref[...] = total
    total = None
    for k, ref in enumerate((own_ref, mate_ref)):
        for far in range(2):
            spot = (flat % 4) ^ k ^ (2 * far)
            at = pl.ds(pl.multiple_of(spot * quarter, quarter), quarter)
            low = half + far * quarter
            term = fine(ref[low : low + quarter, :], b_ref[at, :], ((0,), (0,)))
            total = term if total is None else total + term
    a_ref[...] = total
    keep_ref[...] = a_ref[pl.ds(pl.multiple_of(parity * half, half), half), :]
    send_ref[...] = a_ref[pl.ds(pl.multiple_of((1 - parity) * half, half), half), :]


def far_points_kernel(nodes, flat_ref, lists_ref, own_ref, mate_ref, out_ref, pts_ref):
    flat = flat_ref[0]
    rows = own_ref.shape[2]
    rank = rows * NODE
    node, position = flat // NODE, flat % NODE
    for k, ref in enumerate((own_ref, mate_ref)):
        for m in range(nodes):
            for r in range(NODE // 2):
                at = (node ^ m) * rank + (position ^ (2 * r) ^ k) * rows
                pts_ref[pl.ds(pl.multiple_of(at, rows), rows), :] = ref[m, r].astype(F32)
    feats = pts_ref.shape[1]
    left = pts_ref[pl.ds(pl.multiple_of(node * rank, rank), rank), :].astype(BF16)
    length, inv = norms(left)
    for m in range(nodes):
        at = pl.ds(m * rank, rank)
        pts = pts_ref[at, :]
        row = fine(jnp.ones((8, feats), F32), pts * pts, ((1,), (1,)))
        square = jnp.maximum(row[0:1, :], TINY)
        back = lax.rsqrt(square)
        c = dot(left, pts.astype(BF16), ((1,), (1,)))
        scale = jnp.where(listed(lists_ref, node, m), 0.5, 0.0)
        out_ref[:, m * rank : (m + 1) * rank] = unit_kernel(c * inv * back) * (
            length * (square * back * scale)
        )


def far_kernel(
    nodes, flat_ref, kern_ref, v_ref, vm_ref, b1_ref, own_ref, mate_ref, turned_ref, out_ref,
    w_ref, a_ref, b_ref
):
    flat = flat_ref[0]
    rank = b1_ref.shape[1]
    half, quarter = rank // 2, rank // 4
    node, parity = flat // NODE, flat % 2
    for m in range(nodes):
        for k, ref in enumerate((v_ref, vm_ref)):
            at = (node ^ m) * rank + (parity ^ k) * half
            w_ref[pl.ds(pl.multiple_of(at, half), half), :] = ref[m]
    up = fine(kern_ref[...], w_ref[...])
    for k, ref in enumerate((own_ref, mate_ref)):
        for far in range(2):
            spot = (flat % 4) ^ k ^ (2 * far)
            low = half + far * quarter
            a_ref[pl.ds(pl.multiple_of(spot * quarter, quarter), quarter), :] = fine(
                ref[low : low + quarter, :], up
            )
    up = a_ref[...]
    for k, ref in enumerate((own_ref, mate_ref)):
        at = pl.ds(pl.multiple_of((parity ^ k) * half, half), half)
        b_ref[at, :] = fine(ref[0:half, :], up)
    up = fine(b1_ref[...], b_ref[...])
    hi, lo = halves(up)
    top = jnp.concatenate([hi, lo], 1)
    low = jnp.concatenate([hi, jnp.zeros_like(lo)], 1)
    far = dot(turned_ref[...], jnp.concatenate([top, low], 0))
    width = out_ref.shape[1]
    out_ref[...] = far[:, 0:width] + far[:, width:]


def join_kernel(a_ref, b_ref, c_ref, out_ref):
    out_ref[...] = a_ref[...] + b_ref[...] + c_ref[...]


def body(
    points, rhs, permutation, leaf_basis, climb_leaf, climb_pair, climb_quad, skel_points,
    near_lists, far_lists
):
    size, feats = points.shape
    width = rhs.shape[1]
    rank = climb_leaf.shape[1]
    nodes = lax.axis_size(AXES) // NODE
    flat = lax.axis_index(AXES).astype(jnp.int32).reshape(1)
    struct = jax.ShapeDtypeStruct

    mate_pts = across(points, 1)
    pack_shape = struct((size // 2 + 32, max(feats + 2 * width, size // 2)), BF16)
    pack_a, pack_b = call(pack_kernel, [pack_shape, pack_shape], 0, (points, rhs))
    x_a, y_a = across(pack_a, 2), across(pack_a, 4)
    x_b, y_b = across(pack_b, 2), across(pack_b, 4)
    d_a = across(y_a, 2)
    d_b = across(x_b, 4)

    rows = skel_points.shape[0]
    quad_pts = across(jnp.concatenate([climb_quad, skel_points.astype(F32)], 0), 2)
    own_climb = jnp.concatenate([climb_pair, climb_quad, quad_pts[: rank // 4]], 0)
    mate_climb = across(own_climb, 1)
    two = jnp.stack([skel_points, quad_pts[rank // 4 :].astype(BF16)])
    four = jnp.concatenate([two, across(two, 4)], 0)
    own_skel = jnp.stack([four] + [across(four, NODE * m) for m in range(1, nodes)])
    mate_skel = across(own_skel, 1)

    block = 2 * size * size * (feats + 6 * width) * 4
    sums = struct((size, width), F32)

    def near(masks, packs, before):
        kernel = functools.partial(near_kernel, masks, not before)
        return call(
            kernel, [sums, sums], 2, (flat, near_lists, points, mate_pts, *packs, *before),
            flops=block * len(masks) // 2,
        )

    turned, part = call(
        basis_kernel,
        [struct((size, 2 * rank), BF16), struct((rank, width), F32)],
        0,
        (permutation.reshape(1, size), leaf_basis, rhs, climb_leaf),
        [pltpu.VMEM((size, size), BF16)],
        flops=2 * size * size * rank * 6,
    )
    strip = struct((rank // 2, width), F32)
    keep, send = call(
        climb_kernel, [strip, strip], 1, (flat, part, own_climb, mate_climb),
        [pltpu.VMEM((rank, width), F32), pltpu.VMEM((rank, width), F32)],
        flops=2 * rank * rank * width * 12,
    )
    value = keep + across(send, 1)
    value = value + across(value, 2)
    value = value + across(value, 4)
    every = jnp.stack([value] + [across(value, NODE * m) for m in range(1, nodes)])
    every_mate = across(every, 1)

    kern = call(
        functools.partial(far_points_kernel, nodes),
        struct((rank, nodes * rank), F32),
        2,
        (flat, far_lists, own_skel, mate_skel),
        [pltpu.VMEM((nodes * rank, feats), F32)],
        flops=2 * rank * rank * feats * nodes * 4,
    )

    total = near((0, 0), (pack_a, pack_b), ())
    total = near((2, 4), (x_a, y_a), total)
    total = near((2, 4), (x_b, y_b), total)
    far = call(
        functools.partial(far_kernel, nodes),
        sums,
        1,
        (flat, kern, every, every_mate, climb_leaf, own_climb, mate_climb, turned),
        [
            pltpu.VMEM((nodes * rank, width), F32),
            pltpu.VMEM((rank, width), F32),
            pltpu.VMEM((rank, width), F32),
        ],
        flops=2 * rank * rank * width * 60,
    )
    mine, other = near((6, 6), (d_a, d_b), total)
    return call(join_kernel, sums, 0, (mine, across(other, 1), far))


def solution(mesh):
    split = P(AXES, None)
    return jax.shard_map(
        body,
        mesh=mesh,
        in_specs=(split, split, P(AXES), split, split, split, split, split, P(), P()),
        out_specs=split,
        check_vma=False,
    )
```

```python
import functools

import jax
import jax.numpy as jnp
from jax import lax
from jax.experimental import pallas as pl
from jax.experimental.pallas import tpu as pltpu
from jax.sharding import PartitionSpec as P


AXES = ("leaf", "grp")
NODE = 8
TINY = 1e-30
SERIES = (
    1.0000005285886142,
    -5.669123056911696e-05,
    -0.4990002868296516,
    0.20543817481505877,
    -0.10204939882030772,
    0.040449241962581796,
    -0.008162324706047165,
)
F32 = jnp.float32
BF16 = jnp.bfloat16
HIGHEST = lax.Precision.HIGHEST
VMEM = pltpu.VMEM
SMEM = pltpu.SMEM


def across(value, mask):
    pairs = [(s, s ^ mask) for s in range(lax.axis_size(AXES))]
    return lax.ppermute(value, AXES, pairs)


def call(kernel, out, n_smem, operands, scratch=(), flops=0, aliases=None):
    specs = [pl.BlockSpec(memory_space=SMEM)] * n_smem
    specs += [pl.BlockSpec(memory_space=VMEM)] * (len(operands) - n_smem)
    multi = isinstance(out, (list, tuple))
    return pl.pallas_call(
        kernel,
        out_shape=out,
        in_specs=specs,
        out_specs=[pl.BlockSpec(memory_space=VMEM)] * len(out)
        if multi
        else pl.BlockSpec(memory_space=VMEM),
        scratch_shapes=list(scratch),
        cost_estimate=pl.CostEstimate(flops=flops, bytes_accessed=0, transcendentals=0),
        compiler_params=pltpu.CompilerParams(vmem_limit_bytes=40 * 2**20),
        input_output_aliases=aliases or {},
    )(*operands)


def halves(value):
    hi = value.astype(BF16)
    return hi, (value - hi.astype(F32)).astype(BF16)


def dot(a, b, dims=((1,), (0,))):
    return lax.dot_general(a, b, (dims, ((), ())), preferred_element_type=F32)


def fine(a, b, dims=((1,), (0,))):
    return lax.dot_general(
        a, b, (dims, ((), ())), precision=HIGHEST, preferred_element_type=F32
    )


def unit_kernel(cosine):
    z = jnp.maximum(1.0 - cosine * cosine, TINY)
    w = z * lax.rsqrt(z)
    acc = jnp.full_like(w, SERIES[-1])
    for coef in SERIES[-2::-1]:
        acc = acc * w + coef
    return acc + cosine


def norms(x):
    x = x.astype(F32)
    sq = jnp.maximum(jnp.sum(x * x, axis=1, keepdims=True), TINY)
    inv = lax.rsqrt(sq)
    return sq * inv, inv


def pack_kernel(x_ref, w_ref, a_ref, b_ref):
    half = x_ref.shape[0] // 2
    width = w_ref.shape[1]
    feats = x_ref.shape[1]
    for k, ref in enumerate((a_ref, b_ref)):
        rows = pl.ds(k * half, half)
        x = x_ref[rows, :]
        ref[0:half, 0:feats] = x
        xf = x.astype(F32)
        length, _ = norms(x)
        hi, lo = halves(w_ref[rows, :] * (length * 0.5))
        ref[0:half, feats : feats + width] = hi
        ref[0:half, feats + width : feats + 2 * width] = lo
        row = fine(jnp.ones((8, feats), F32), xf * xf, ((1,), (1,)))
        inv = lax.rsqrt(jnp.maximum(row, TINY))
        p0 = inv.astype(BF16)
        rest = inv - p0.astype(F32)
        p1 = rest.astype(BF16)
        p2 = (rest - p1.astype(F32)).astype(BF16)
        wide = jnp.zeros((8, ref.shape[1] - half), BF16)
        if wide.shape[1]:
            p0, p1, p2 = (jnp.concatenate([p, wide], 1) for p in (p0, p1, p2))
        ref[half : half + 8, :] = p0
        ref[half + 8 : half + 16, :] = p1
        ref[half + 16 : half + 24, :] = p2
        ref[half + 24 : half + 32, :] = jnp.zeros_like(p0)


def listed(lists_ref, row, value):
    hit = lists_ref[row, 0] == value
    for s in range(1, lists_ref.shape[1]):
        hit = jnp.logical_or(hit, lists_ref[row, s] == value)
    return hit


def near_kernel(masks, first, last, *refs):
    count = len(masks)
    flat_ref, lists_ref, own_ref, mate_ref = refs[:4]
    packs = refs[4 : 4 + count]
    x_ref, p_ref, n_ref, acc_ref, todo_ref = refs[-5:]
    outs = refs[-5 - (2 if last else 1) : -5]
    flat = flat_ref[0]
    size, feats = own_ref.shape
    half = size // 2
    width = acc_ref.shape[2]
    tile = 128
    x_ref[0] = own_ref[...]
    x_ref[1] = mate_ref[...]
    for k, pack in enumerate(packs):
        p_ref[k] = pack[...]
    acc_ref[...] = jnp.zeros_like(acc_ref) if first else refs[4 + count][...]
    for t in range(2):
        for k, mask in enumerate(masks):
            hit = listed(lists_ref, flat ^ t, flat ^ mask)
            todo_ref[t * count + k] = hit.astype(jnp.int32)

    def job(index, carry):
        t = index // count
        k = index % count

        @pl.when(jnp.logical_and(todo_ref[index] > 0, carry != t))
        def _():
            for i in range(size // 256):
                at = pl.ds(i * 256, 256)
                length, inv = norms(x_ref[t, at, :])
                n_ref[0, at, :] = length
                n_ref[1, at, :] = inv

        @pl.when(todo_ref[index] > 0)
        def _():
            inv_row = (
                p_ref[k, half : half + 8, 0:half].astype(F32)
                + p_ref[k, half + 8 : half + 16, 0:half].astype(F32)
                + p_ref[k, half + 16 : half + 24, 0:half].astype(F32)
            )[0:1, :]
            weights = p_ref[k, 0:half, feats : feats + 2 * width]
            for i in range(size // tile):
                at = pl.ds(i * tile, tile)
                c = dot(x_ref[t, at, :], p_ref[k, 0:half, 0:feats], ((1,), (1,)))
                hi, lo = halves(unit_kernel(c * n_ref[1, at, :] * inv_row))
                total = dot(hi, weights) + dot(lo, weights)
                acc_ref[t, at, :] += n_ref[0, at, :] * (total[:, 0:width] + total[:, width:])

        return jnp.where(todo_ref[index] > 0, t, carry)

    lax.fori_loop(0, 2 * count, job, -1)
    if last:
        outs[0][...] = acc_ref[0]
        outs[1][...] = acc_ref[1]
    else:
        outs[0][...] = acc_ref[...]


def basis_kernel(perm_ref, basis_ref, w_ref, first_ref, turned_ref, part_ref, hot_ref):
    size = basis_ref.shape[1]
    rank = basis_ref.shape[0]
    width = w_ref.shape[1]
    place = lax.rem(perm_ref[...], size)
    for i in range(size // 256):
        spot = lax.broadcasted_iota(jnp.int32, (256, size), 0) + i * 256
        hot_ref[i * 256 : (i + 1) * 256, :] = jnp.where(spot == place, 1.0, 0.0).astype(BF16)
    hi, lo = halves(basis_ref[...])
    pair = jnp.concatenate([hi, lo], 0)
    hot = hot_ref[...]
    turned_ref[...] = dot(hot, pair, ((1,), (1,))).astype(BF16)
    moved = dot(pair, hot, ((1,), (1,))).astype(BF16)
    whi, wlo = halves(w_ref[...])
    y = dot(moved, jnp.concatenate([whi, wlo], 1))
    y = y[0:rank, 0:width] + y[0:rank, width:] + y[rank:, 0:width]
    part_ref[...] = fine(first_ref[...], y, ((0,), (0,)))


def climb_kernel(flat_ref, part_ref, *refs):
    pairs, quads = refs[0:2], refs[2:6]
    keep_ref, send_ref, a_ref, b_ref = refs[6:]
    flat = flat_ref[0]
    half, quarter = pairs[0].shape[0], quads[0].shape[0]
    parity = flat % 2
    a_ref[...] = part_ref[...]
    total = None
    for k, ref in enumerate(pairs):
        at = pl.ds(pl.multiple_of((parity ^ k) * half, half), half)
        term = fine(ref[...], a_ref[at, :], ((0,), (0,)))
        total = term if total is None else total + term
    b_ref[...] = total
    total = None
    for k, ref in enumerate(quads):
        at = pl.ds(pl.multiple_of(((flat % 4) ^ k) * quarter, quarter), quarter)
        term = fine(ref[...], b_ref[at, :], ((0,), (0,)))
        total = term if total is None else total + term
    a_ref[...] = total
    keep_ref[...] = a_ref[pl.ds(pl.multiple_of(parity * half, half), half), :]
    send_ref[...] = a_ref[pl.ds(pl.multiple_of((1 - parity) * half, half), half), :]


def far_points_kernel(nodes, flat_ref, lists_ref, own_ref, mate_ref, out_ref, pts_ref):
    flat = flat_ref[0]
    rows = own_ref.shape[2]
    rank = rows * NODE
    node, position = flat // NODE, flat % NODE
    for k, ref in enumerate((own_ref, mate_ref)):
        for m in range(nodes):
            for r in range(NODE // 2):
                at = (node ^ m) * rank + (position ^ (2 * r) ^ k) * rows
                pts_ref[pl.ds(pl.multiple_of(at, rows), rows), :] = ref[m, r].astype(F32)
    feats = pts_ref.shape[1]
    left = pts_ref[pl.ds(pl.multiple_of(node * rank, rank), rank), :].astype(BF16)
    length, inv = norms(left)
    for m in range(nodes):
        at = pl.ds(m * rank, rank)
        pts = pts_ref[at, :]
        row = fine(jnp.ones((8, feats), F32), pts * pts, ((1,), (1,)))
        square = jnp.maximum(row[0:1, :], TINY)
        back = lax.rsqrt(square)
        c = dot(left, pts.astype(BF16), ((1,), (1,)))
        scale = jnp.where(listed(lists_ref, node, m), 0.5, 0.0)
        out_ref[:, m * rank : (m + 1) * rank] = unit_kernel(c * inv * back) * (
            length * (square * back * scale)
        )


def far_kernel(nodes, flat_ref, kern_ref, v_ref, vm_ref, b1_ref, *refs):
    pairs, quads = refs[0:2], refs[2:6]
    turned_ref, out_ref, w_ref, a_ref, b_ref = refs[6:]
    flat = flat_ref[0]
    rank = b1_ref.shape[1]
    half, quarter = pairs[0].shape[0], quads[0].shape[0]
    node, parity = flat // NODE, flat % 2
    for m in range(nodes):
        for k, ref in enumerate((v_ref, vm_ref)):
            at = (node ^ m) * rank + (parity ^ k) * half
            w_ref[pl.ds(pl.multiple_of(at, half), half), :] = ref[m]
    up = fine(kern_ref[...], w_ref[...])
    for k, ref in enumerate(quads):
        at = pl.ds(pl.multiple_of(((flat % 4) ^ k) * quarter, quarter), quarter)
        a_ref[at, :] = fine(ref[...], up)
    up = a_ref[...]
    for k, ref in enumerate(pairs):
        at = pl.ds(pl.multiple_of((parity ^ k) * half, half), half)
        b_ref[at, :] = fine(ref[...], up)
    up = fine(b1_ref[...], b_ref[...])
    hi, lo = halves(up)
    top = jnp.concatenate([hi, lo], 1)
    low = jnp.concatenate([hi, jnp.zeros_like(lo)], 1)
    far = dot(turned_ref[...], jnp.concatenate([top, low], 0))
    width = out_ref.shape[1]
    out_ref[...] = far[:, 0:width] + far[:, width:]


def join_kernel(a_ref, b_ref, c_ref, out_ref):
    out_ref[...] = a_ref[...] + b_ref[...] + c_ref[...]


def body(
    points, rhs, permutation, leaf_basis, climb_leaf, climb_pair, climb_quad, skel_points,
    near_lists, far_lists
):
    size, feats = points.shape
    width = rhs.shape[1]
    rank = climb_leaf.shape[1]
    nodes = lax.axis_size(AXES) // NODE
    flat = lax.axis_index(AXES).astype(jnp.int32).reshape(1)
    struct = jax.ShapeDtypeStruct

    quads = [climb_quad] + [across(climb_quad, k) for k in (1, 2, 3)]
    pairs = [climb_pair, across(climb_pair, 1)]
    four = jnp.stack([skel_points] + [across(skel_points, k) for k in (2, 4, 6)])

    mate_pts = across(points, 1)
    pack_shape = struct((size // 2 + 32, max(feats + 2 * width, size // 2)), BF16)
    pack_a, pack_b = call(pack_kernel, [pack_shape, pack_shape], 0, (points, rhs))
    x_a, y_a = across(pack_a, 2), across(pack_a, 4)
    x_b, y_b = across(pack_b, 2), across(pack_b, 4)
    d_a = across(y_a, 2)
    d_b = across(x_b, 4)
    masks = [NODE * m for m in range(1, nodes)]
    own_skel = jnp.stack([four] + [across(four, m) for m in masks])
    mate_skel = across(own_skel, 1)

    block = 2 * size * size * (feats + 6 * width) * 4
    sums = struct((size, width), F32)

    def near(masks, packs, before, last=False):
        kernel = functools.partial(near_kernel, masks, before is None, last)
        before = () if before is None else (before,)
        return call(
            kernel, [sums, sums] if last else struct((2, size, width), F32), 2,
            (flat, near_lists, points, mate_pts, *packs, *before),
            [
                pltpu.VMEM((2, size, feats), BF16),
                pltpu.VMEM((len(masks), *pack_shape.shape), BF16),
                pltpu.VMEM((2, size, 1), F32),
                pltpu.VMEM((2, size, width), F32),
                pltpu.SMEM((2 * len(masks),), jnp.int32),
            ],
            flops=block * len(masks) // 2,
        )

    turned, part = call(
        basis_kernel,
        [struct((size, 2 * rank), BF16), struct((rank, width), F32)],
        0,
        (permutation.reshape(1, size), leaf_basis, rhs, climb_leaf),
        [pltpu.VMEM((size, size), BF16)],
        flops=2 * size * size * rank * 6,
    )
    strip = struct((rank // 2, width), F32)
    keep, send = call(
        climb_kernel, [strip, strip], 1, (flat, part, *pairs, *quads),
        [pltpu.VMEM((rank, width), F32), pltpu.VMEM((rank, width), F32)],
        flops=2 * rank * rank * width * 12,
    )
    value = keep + across(send, 1)
    value = (value + across(value, 2)) + (across(value, 4) + across(value, 6))
    every = jnp.stack([value] + [across(value, m) for m in masks])
    every_mate = across(every, 1)

    kern = call(
        functools.partial(far_points_kernel, nodes),
        struct((rank, nodes * rank), F32),
        2,
        (flat, far_lists, own_skel, mate_skel),
        [pltpu.VMEM((nodes * rank, feats), F32)],
        flops=2 * rank * rank * feats * nodes * 4,
    )

    total = near((0, 0), (pack_a, pack_b), None)
    total = near((2, 4), (x_a, y_a), total)
    total = near((2, 4), (x_b, y_b), total)
    far = call(
        functools.partial(far_kernel, nodes),
        sums,
        1,
        (flat, kern, every, every_mate, climb_leaf, *pairs, *quads, turned),
        [
            pltpu.VMEM((nodes * rank, width), F32),
            pltpu.VMEM((rank, width), F32),
            pltpu.VMEM((rank, width), F32),
        ],
        flops=2 * rank * rank * width * 60,
    )
    mine, other = near((6, 6), (d_a, d_b), total, True)
    return call(join_kernel, sums, 0, (mine, across(other, 1), far))


def solution(mesh):
    split = P(AXES, None)

    return jax.shard_map(
        body,
        mesh=mesh,
        in_specs=(split, split, P(AXES), split, split, split, split, split, P(), P()),
        out_specs=split,
        check_vma=False,
    )
```

```python
import functools

import jax
import jax.numpy as jnp
from jax import lax
from jax.experimental import pallas as pl
from jax.experimental.pallas import tpu as pltpu
from jax.sharding import PartitionSpec as P


AXES = ("leaf", "grp")
NODE = 8
TINY = 1e-30
SERIES = (
    1.0000005285886142,
    -5.669123056911696e-05,
    -0.4990002868296516,
    0.20543817481505877,
    -0.10204939882030772,
    0.040449241962581796,
    -0.008162324706047165,
)
F32 = jnp.float32
BF16 = jnp.bfloat16
VMEM = pltpu.VMEM
SMEM = pltpu.SMEM


def across(value, mask):
    pairs = [(s, s ^ mask) for s in range(lax.axis_size(AXES))]
    return lax.ppermute(value, AXES, pairs)


def call(kernel, out, n_smem, operands, scratch=(), flops=0, loose=0,
         far_memory=False):
    specs = [pl.BlockSpec(memory_space=SMEM)] * n_smem
    specs += [pl.BlockSpec(memory_space=pltpu.MemorySpace.HBM if far_memory else pl.ANY)] * loose
    specs += [pl.BlockSpec(memory_space=VMEM)] * (len(operands) - n_smem - loose)
    multi = isinstance(out, (list, tuple))
    return pl.pallas_call(
        kernel,
        out_shape=out,
        in_specs=specs,
        out_specs=[pl.BlockSpec(memory_space=VMEM)] * len(out)
        if multi
        else pl.BlockSpec(memory_space=VMEM),
        scratch_shapes=list(scratch),
        cost_estimate=pl.CostEstimate(flops=flops, bytes_accessed=0, transcendentals=0),
        compiler_params=pltpu.CompilerParams(vmem_limit_bytes=40 * 2**20),
    )(*operands)


def halves(value):
    hi = value.astype(BF16)
    return hi, (value - hi.astype(F32)).astype(BF16)


def dot(a, b, dims=((1,), (0,))):
    return lax.dot_general(a, b, (dims, ((), ())), preferred_element_type=F32)


def three(a, b, dims=((1,), (0,))):
    ahi, alo = halves(a)
    wide = jnp.concatenate(halves(b), 1)
    width = b.shape[1]
    total = dot(ahi, wide, dims) + dot(alo, wide, dims)
    return total[:, 0:width] + total[:, width:]


def unit_kernel(cosine):
    z = jnp.maximum(1.0 - cosine * cosine, TINY)
    w = z * lax.rsqrt(z)
    acc = jnp.full_like(w, SERIES[-1])
    for coef in SERIES[-2::-1]:
        acc = acc * w + coef
    return acc + cosine


def norms(x):
    x = x.astype(F32)
    sq = jnp.maximum(jnp.sum(x * x, axis=1, keepdims=True), TINY)
    inv = lax.rsqrt(sq)
    return sq * inv, inv


def pack_kernel(x_hbm, w_hbm, a_ref, b_ref, x_ref, w_ref, sem):
    half = x_ref.shape[0] // 2
    width = w_ref.shape[1]
    feats = x_ref.shape[1]
    moves = []
    for k in range(2):
        rows = pl.ds(k * half, half)
        for j, (src, dst) in enumerate(((x_hbm, x_ref), (w_hbm, w_ref))):
            move = pltpu.make_async_copy(src.at[rows, :], dst.at[rows, :], sem.at[2 * k + j])
            move.start()
            moves.append(move)
    for k, ref in enumerate((a_ref, b_ref)):
        rows = pl.ds(k * half, half)
        moves[2 * k].wait()
        moves[2 * k + 1].wait()
        x = x_ref[rows, :]
        ref[0:half, 0:feats] = x
        xf = x.astype(F32)
        length, _ = norms(x)
        hi, lo = halves(w_ref[rows, :] * (length * 0.5))
        ref[0:half, feats : feats + width] = hi
        ref[0:half, feats + width : feats + 2 * width] = lo
        shi, slo = halves(xf * xf)
        ones = jnp.ones((8, feats), BF16)
        row = dot(ones, shi, ((1,), (1,))) + dot(ones, slo, ((1,), (1,)))
        inv = lax.rsqrt(jnp.maximum(row, TINY))
        p0 = inv.astype(BF16)
        rest = inv - p0.astype(F32)
        p1 = rest.astype(BF16)
        p2 = (rest - p1.astype(F32)).astype(BF16)
        wide = jnp.zeros((8, ref.shape[1] - half), BF16)
        if wide.shape[1]:
            p0, p1, p2 = (jnp.concatenate([p, wide], 1) for p in (p0, p1, p2))
        ref[half : half + 8, :] = p0
        ref[half + 8 : half + 16, :] = p1
        ref[half + 16 : half + 24, :] = p2
        ref[half + 24 : half + 32, :] = jnp.zeros_like(p0)


def listed(lists_ref, row, value):
    hit = lists_ref[row, 0] == value
    for s in range(1, lists_ref.shape[1]):
        hit = jnp.logical_or(hit, lists_ref[row, s] == value)
    return hit


def near_kernel(masks, jobs, first, last, *refs):
    count = len(masks)
    sides = 1 + max(t for t, _ in jobs)
    flat_ref, lists_ref = refs[:2]
    targets = refs[2 : 2 + sides]
    packs = refs[2 + sides : 2 + sides + count]
    x_ref, p_ref, n_ref, acc_ref, todo_ref, x_sem, p_sem = refs[-7:]
    outs = refs[-7 - (2 if last else 1) : -7]
    flat = flat_ref[0]
    size, feats = targets[0].shape
    half = size // 2
    width = outs[0].shape[-1]
    tile = 128
    if not last:
        acc_ref = outs[0]
    hits = [listed(lists_ref, flat ^ t, flat ^ masks[k]).astype(jnp.int32) for t, k in jobs]
    for i, (t, k) in enumerate(jobs):
        todo_ref[0, i] = hits[i]
        todo_ref[1, i] = jnp.int32(t)
        todo_ref[2, i] = jnp.int32(k)
    moves = []
    for t in range(sides):
        need = sum(hit for hit, job in zip(hits, jobs) if job[0] == t)
        moves.append((need, pltpu.make_async_copy(targets[t], x_ref.at[t], x_sem.at[t])))
    for k in range(count):
        need = sum(hit for hit, job in zip(hits, jobs) if job[1] == k)
        moves.append((need, pltpu.make_async_copy(packs[k], p_ref.at[k], p_sem.at[k])))
    for i, (t, k) in enumerate(jobs):
        fresh = hits[i]
        for before, job in zip(hits[:i], jobs[:i]):
            if job[1] == k:
                fresh = fresh * (1 - before)
        todo_ref[3, i] = fresh
    for need, move in moves:
        pl.when(need > 0)(move.start)
    acc_ref[...] = jnp.zeros_like(acc_ref) if first else refs[2 + sides + count][...]

    def job(index, carry):
        active = todo_ref[0, index] > 0
        t = todo_ref[1, index]
        k = todo_ref[2, index]

        for side in range(sides):
            pl.when(active & (carry != t) & (t == side))(moves[side][1].wait)
        for pack in range(count):
            pl.when((todo_ref[3, index] > 0) & (k == pack))(moves[sides + pack][1].wait)

        @pl.when(jnp.logical_and(active, carry != t))
        def _():
            for i in range(size // 256):
                at = pl.ds(i * 256, 256)
                length, inv = norms(x_ref[t, at, :])
                n_ref[0, at, :] = length
                n_ref[1, at, :] = inv

        @pl.when(active)
        def _():
            inv_row = (
                p_ref[k, half : half + 8, 0:half].astype(F32)
                + p_ref[k, half + 8 : half + 16, 0:half].astype(F32)
                + p_ref[k, half + 16 : half + 24, 0:half].astype(F32)
            )[0:1, :]
            weights = p_ref[k, 0:half, feats : feats + 2 * width]
            for i in range(size // tile):
                at = pl.ds(i * tile, tile)
                c = dot(x_ref[t, at, :], p_ref[k, 0:half, 0:feats], ((1,), (1,)))
                hi, lo = halves(unit_kernel(c * n_ref[1, at, :] * inv_row))
                total = dot(hi, weights) + dot(lo, weights)
                acc_ref[t, at, :] += n_ref[0, at, :] * (total[:, 0:width] + total[:, width:])

        return jnp.where(active, t, carry)

    lax.fori_loop(0, len(jobs), job, -1)
    if last:
        outs[0][...] = acc_ref[0]
        outs[1][...] = acc_ref[1]


def basis_kernel(
    basis_hbm, w_hbm, first_hbm, perm_ref, turned_ref, part_ref, hot_ref, basis_ref, w_ref,
    first_ref, sem
):
    moves = []
    for k, (src, dst) in enumerate(
        ((basis_hbm, basis_ref), (w_hbm, w_ref), (first_hbm, first_ref))
    ):
        moves.append(pltpu.make_async_copy(src, dst, sem.at[k]))
        moves[k].start()
    size = basis_ref.shape[1]
    rank = basis_ref.shape[0]
    width = w_ref.shape[1]
    place = lax.rem(perm_ref[...], size)
    for i in range(size // 256):
        spot = lax.broadcasted_iota(jnp.int32, (256, size), 0) + i * 256
        hot_ref[i * 256 : (i + 1) * 256, :] = jnp.where(spot == place, 1.0, 0.0).astype(BF16)
    for move in moves:
        move.wait()
    hi, lo = halves(basis_ref[...])
    pair = jnp.concatenate([hi, lo], 0)
    hot = hot_ref[...]
    turned_ref[...] = dot(hot, pair, ((1,), (1,))).astype(BF16)
    moved = dot(pair, hot, ((1,), (1,))).astype(BF16)
    whi, wlo = halves(w_ref[...])
    y = dot(moved, jnp.concatenate([whi, wlo], 1))
    y = y[0:rank, 0:width] + y[0:rank, width:] + y[rank:, 0:width]
    part_ref[...] = three(first_ref[...], y, ((0,), (0,)))


def climb_kernel(flat_ref, part_ref, *refs):
    pairs, quads = refs[0:2], refs[2:6]
    keep_ref, send_ref, a_ref, b_ref = refs[6:]
    flat = flat_ref[0]
    half, quarter = pairs[0].shape[0], quads[0].shape[0]
    parity = flat % 2
    a_ref[...] = part_ref[...]
    total = None
    for k, ref in enumerate(pairs):
        at = pl.ds(pl.multiple_of((parity ^ k) * half, half), half)
        term = three(ref[...], a_ref[at, :], ((0,), (0,)))
        total = term if total is None else total + term
    b_ref[...] = total
    total = None
    for k, ref in enumerate(quads):
        at = pl.ds(pl.multiple_of(((flat % 4) ^ k) * quarter, quarter), quarter)
        term = three(ref[...], b_ref[at, :], ((0,), (0,)))
        total = term if total is None else total + term
    a_ref[...] = total
    keep_ref[...] = a_ref[pl.ds(pl.multiple_of(parity * half, half), half), :]
    send_ref[...] = a_ref[pl.ds(pl.multiple_of((1 - parity) * half, half), half), :]


def mate_sum_kernel(keep_ref, got_ref, pts_ref, out_ref):
    hi, lo = halves(keep_ref[...] + got_ref[...])
    half, width = keep_ref.shape
    out_ref[0:half, 0:width] = hi
    out_ref[0:half, width:] = lo
    out_ref[half:, :] = pts_ref[...]


def node_sum_kernel(*refs):
    ins, out_ref = refs[:-1], refs[-1]
    rows = (out_ref.shape[0] - ins[0].shape[0]) // (len(ins) - 1)
    half = ins[0].shape[0] - rows
    width = ins[0].shape[1] // 2
    total = None
    for k, ref in enumerate(ins):
        term = ref[0:half, 0:width].astype(F32) + ref[0:half, width:].astype(F32)
        total = term if total is None else total + term
        out_ref[half + k * rows : half + (k + 1) * rows, :] = ref[half:, :]
    hi, lo = halves(total)
    out_ref[0:half, 0:width] = hi
    out_ref[0:half, width:] = lo


def far_kernel(nodes, flat_ref, lists_ref, own_ref, mate_ref, b1_ref, *refs):
    pairs, quads = refs[0:2], refs[2:6]
    turned_ref, out_ref, pts_ref, w_ref, a_ref, b_ref = refs[6:]
    flat = flat_ref[0]
    rank = b1_ref.shape[1]
    half, quarter = pairs[0].shape[0], quads[0].shape[0]
    node, position, parity = flat // NODE, flat % NODE, flat % 2
    width = out_ref.shape[1]
    rows = rank // NODE
    for k, ref in enumerate((own_ref, mate_ref)):
        for m in range(nodes):
            at = (node ^ m) * rank + (parity ^ k) * half
            w_ref[pl.ds(pl.multiple_of(at, half), half), :] = ref[m, 0:half, :]
            for r in range(NODE // 2):
                at = (node ^ m) * rank + (position ^ (2 * r) ^ k) * rows
                low = half + r * rows
                pts_ref[pl.ds(pl.multiple_of(at, rows), rows), :] = ref[m, low : low + rows, :]
    feats = pts_ref.shape[1]
    left = pts_ref[pl.ds(pl.multiple_of(node * rank, rank), rank), :]
    length, inv = norms(left)
    up = jnp.zeros((rank, 2 * width), F32)
    for m in range(nodes):
        at = pl.ds(m * rank, rank)
        pts = pts_ref[at, :]
        wide = pts.astype(F32)
        shi, slo = halves(wide * wide)
        ones = jnp.ones((8, feats), BF16)
        row = dot(ones, shi, ((1,), (1,))) + dot(ones, slo, ((1,), (1,)))
        square = jnp.maximum(row[0:1, :], TINY)
        back = lax.rsqrt(square)
        c = dot(left, pts, ((1,), (1,)))
        scale = jnp.where(listed(lists_ref, node, m), 0.5, 0.0)
        hi, lo = halves(unit_kernel(c * inv * back) * (square * back * scale))
        up = up + dot(hi, w_ref[at, :]) + dot(lo, w_ref[at, :])
    up = length * (up[:, 0:width] + up[:, width:])
    for k, ref in enumerate(quads):
        at = pl.ds(pl.multiple_of(((flat % 4) ^ k) * quarter, quarter), quarter)
        a_ref[at, :] = three(ref[...], up)
    up = a_ref[...]
    for k, ref in enumerate(pairs):
        at = pl.ds(pl.multiple_of((parity ^ k) * half, half), half)
        b_ref[at, :] = three(ref[...], up)
    up = three(b1_ref[...], b_ref[...])
    hi, lo = halves(up)
    top = jnp.concatenate([hi, lo], 1)
    low = jnp.concatenate([hi, jnp.zeros_like(lo)], 1)
    far = dot(turned_ref[...], jnp.concatenate([top, low], 0))
    out_ref[...] = far[:, 0:width] + far[:, width:]


def join_kernel(a_ref, b_ref, c_ref, out_ref):
    out_ref[...] = (a_ref[...] + c_ref[...]) + b_ref[...]


def stack_kernel(*refs):
    for k, ref in enumerate(refs[:-1]):
        refs[-1][k] = ref[...]


def body(
    points, rhs, permutation, leaf_basis, climb_leaf, climb_pair, climb_quad, skel_points,
    near_lists, far_lists
):
    size, feats = points.shape
    width = rhs.shape[1]
    rank = climb_leaf.shape[1]
    nodes = lax.axis_size(AXES) // NODE
    flat = lax.axis_index(AXES).astype(jnp.int32).reshape(1)
    struct = jax.ShapeDtypeStruct

    quads = [climb_quad] + [across(climb_quad, k) for k in (1, 2, 3)]
    pairs = [climb_pair, across(climb_pair, 1)]

    mate_pts = across(points, 1)
    pack_shape = struct((size // 2 + 32, max(feats + 2 * width, size // 2)), BF16)
    pack_a, pack_b = call(
        pack_kernel, [pack_shape, pack_shape], 0, (points, rhs),
        [
            pltpu.VMEM((size, feats), BF16),
            pltpu.VMEM((size, width), F32),
            pltpu.SemaphoreType.DMA((4,)),
        ],
        loose=2,
        far_memory=True,
    )
    x_a, y_a = across(pack_a, 2), across(pack_a, 4)
    x_b, y_b = across(pack_b, 2), across(pack_b, 4)
    d_a = across(y_a, 2)
    d_b = across(x_b, 4)
    masks = [NODE * m for m in range(1, nodes)]

    block = 2 * size * size * (feats + 6 * width) * 4
    sums = struct((size, width), F32)

    def near(masks, jobs, packs, before=None, last=False):
        kernel = functools.partial(near_kernel, masks, jobs, before is None, last)
        before = () if before is None else (before,)
        sides = (points, mate_pts)[: 1 + max(t for t, _ in jobs)]
        loose = len(sides) + len(masks)
        return call(
            kernel, [sums, sums] if last else struct((2, size, width), F32), 2,
            (flat, near_lists, *sides, *packs, *before),
            [
                pltpu.VMEM((len(sides), size, feats), BF16),
                pltpu.VMEM((len(masks), *pack_shape.shape), BF16),
                pltpu.VMEM((2, size, 1), F32),
                pltpu.VMEM((2, size, width) if last else (8, 128), F32),
                pltpu.SMEM((4, len(jobs)), jnp.int32),
                pltpu.SemaphoreType.DMA((len(sides),)),
                pltpu.SemaphoreType.DMA((len(masks),)),
            ],
            flops=block * len(jobs) // 2,
            loose=loose,
        )

    turned, part = call(
        basis_kernel,
        [struct((size, 2 * rank), BF16), struct((rank, width), F32)],
        0,
        (leaf_basis, rhs, climb_leaf, permutation.reshape(1, size)),
        [
            pltpu.VMEM((size, size), BF16),
            pltpu.VMEM((rank, size), F32),
            pltpu.VMEM((size, width), F32),
            pltpu.VMEM((rank, rank), F32),
            pltpu.SemaphoreType.DMA((3,)),
        ],
        loose=3,
        far_memory=True,
        flops=2 * size * size * rank * 6,
    )
    strip = struct((rank // 2, width), F32)
    keep, send = call(
        climb_kernel, [strip, strip], 1, (flat, part, *pairs, *quads),
        [pltpu.VMEM((rank, width), F32), pltpu.VMEM((rank, width), F32)],
        flops=2 * rank * rank * width * 12,
    )
    rows = rank // 2 + skel_points.shape[0]
    strip = call(
        mate_sum_kernel, struct((rows, 2 * width), BF16), 0,
        (keep, across(send, 1), skel_points),
    )
    strips = [strip] + [across(strip, k) for k in (2, 4, 6)]
    rows = rank // 2 + 4 * skel_points.shape[0]
    value = call(node_sum_kernel, struct((rows, 2 * width), BF16), 0, tuple(strips))
    others = [across(value, m) for m in masks]
    every = call(stack_kernel, struct((nodes, *value.shape), BF16), 0, (value, *others))
    every_mate = across(every, 1)

    own = (pack_a, pack_b)
    total = near((0, 0), ((0, 0), (0, 1)), own)
    total = near((0, 0), ((1, 0), (1, 1)), own, total)
    jobs = [(t, k) for t in range(2) for k in range(4)]
    total = near((2, 2, 4, 4), jobs, (x_a, x_b, y_a, y_b), total)
    jobs = ((0, 0), (0, 1), (1, 0), (1, 1))
    mine, other = near((6, 6), jobs, (d_a, d_b), total, True)
    far = call(
        functools.partial(far_kernel, nodes),
        sums,
        2,
        (
            flat, far_lists, every, every_mate, climb_leaf, *pairs, *quads, turned
        ),
        [
            pltpu.VMEM((nodes * rank, feats), BF16),
            pltpu.VMEM((nodes * rank, 2 * width), BF16),
            pltpu.VMEM((rank, width), F32),
            pltpu.VMEM((rank, width), F32),
        ],
        flops=2 * rank * rank * width * 60,
    )
    return call(join_kernel, sums, 0, (mine, across(other, 1), far))


def solution(mesh):
    split = P(AXES, None)

    return jax.shard_map(
        body,
        mesh=mesh,
        in_specs=(split, split, P(AXES), split, split, split, split, split, P(), P()),
        out_specs=split,
        check_vma=False,
    )
```

```python
import functools

import jax
import jax.numpy as jnp
from jax import lax
from jax.experimental import pallas as pl
from jax.experimental.pallas import tpu as pltpu
from jax.sharding import PartitionSpec as P


AXES = ("leaf", "grp")
NODE = 8
TINY = 1e-30
SERIES = (
    1.0000005285886142,
    -5.669123056911696e-05,
    -0.4990002868296516,
    0.20543817481505877,
    -0.10204939882030772,
    0.040449241962581796,
    -0.008162324706047165,
)
F32 = jnp.float32
BF16 = jnp.bfloat16
VMEM = pltpu.VMEM
SMEM = pltpu.SMEM


def across(value, mask):
    pairs = [(s, s ^ mask) for s in range(lax.axis_size(AXES))]
    return lax.ppermute(value, AXES, pairs)


def call(kernel, out, n_smem, operands, scratch=(), flops=0, loose=0,
         vmem=16):
    specs = [pl.BlockSpec(memory_space=SMEM)] * n_smem
    specs += [pl.BlockSpec(memory_space=pl.ANY)] * loose
    specs += [pl.BlockSpec(memory_space=VMEM)] * (len(operands) - n_smem - loose)
    multi = isinstance(out, (list, tuple))
    return pl.pallas_call(
        kernel,
        out_shape=out,
        in_specs=specs,
        out_specs=[pl.BlockSpec(memory_space=VMEM)] * len(out)
        if multi
        else pl.BlockSpec(memory_space=VMEM),
        scratch_shapes=list(scratch),
        cost_estimate=pl.CostEstimate(flops=flops, bytes_accessed=0, transcendentals=0),
        compiler_params=pltpu.CompilerParams(vmem_limit_bytes=vmem * 2**20),
    )(*operands)


def halves(value):
    hi = value.astype(BF16)
    return hi, (value - hi.astype(F32)).astype(BF16)


def dot(a, b, dims=((1,), (0,))):
    return lax.dot_general(a, b, (dims, ((), ())), preferred_element_type=F32)


def three(a, b, dims=((1,), (0,))):
    ahi, alo = halves(a)
    wide = jnp.concatenate(halves(b), 1)
    width = b.shape[1]
    total = dot(ahi, wide, dims) + dot(alo, wide, dims)
    return total[:, 0:width] + total[:, width:]


def unit_kernel(cosine):
    z = jnp.maximum(1.0 - cosine * cosine, TINY)
    w = z * lax.rsqrt(z)
    acc = jnp.full_like(w, SERIES[-1])
    for coef in SERIES[-2::-1]:
        acc = acc * w + coef
    return acc + cosine


def norms(x):
    x = x.astype(F32)
    sq = jnp.maximum(jnp.sum(x * x, axis=1, keepdims=True), TINY)
    inv = lax.rsqrt(sq)
    return sq * inv, inv


def pack_kernel(x_hbm, w_hbm, a_ref, b_ref, x_ref, w_ref, sem):
    half = x_ref.shape[0] // 2
    width = w_ref.shape[1]
    feats = x_ref.shape[1]
    moves = []
    for k in range(2):
        rows = pl.ds(k * half, half)
        for j, (src, dst) in enumerate(((x_hbm, x_ref), (w_hbm, w_ref))):
            move = pltpu.make_async_copy(src.at[rows, :], dst.at[rows, :], sem.at[2 * k + j])
            move.start()
            moves.append(move)
    for k, ref in enumerate((a_ref, b_ref)):
        rows = pl.ds(k * half, half)
        moves[2 * k].wait()
        moves[2 * k + 1].wait()
        x = x_ref[rows, :]
        ref[0:half, 0:feats] = x
        xf = x.astype(F32)
        length, _ = norms(x)
        hi, lo = halves(w_ref[rows, :] * (length * 0.5))
        ref[0:half, feats : feats + width] = hi
        ref[0:half, feats + width : feats + 2 * width] = lo
        shi, slo = halves(xf * xf)
        ones = jnp.ones((8, feats), BF16)
        row = dot(ones, shi, ((1,), (1,))) + dot(ones, slo, ((1,), (1,)))
        inv = lax.rsqrt(jnp.maximum(row, TINY))
        p0 = inv.astype(BF16)
        rest = inv - p0.astype(F32)
        p1 = rest.astype(BF16)
        p2 = (rest - p1.astype(F32)).astype(BF16)
        spot = lax.broadcasted_iota(jnp.int32, row.shape, 0)
        parts = jnp.where(spot == 0, p0.astype(F32), jnp.where(spot == 1, p1.astype(F32), 0.0))
        parts = jnp.where(spot == 2, p2.astype(F32), parts)
        parts = jnp.concatenate([parts, jnp.zeros_like(parts)], 0)
        if ref.shape[1] > half:
            wide = jnp.zeros((16, ref.shape[1] - half), F32)
            parts = jnp.concatenate([parts, wide], 1)
        ref[half : half + 16, :] = parts.astype(BF16)


def listed(lists_ref, row, value):
    hit = lists_ref[row, 0] == value
    for s in range(1, lists_ref.shape[1]):
        hit = jnp.logical_or(hit, lists_ref[row, s] == value)
    return hit


def near_kernel(masks, jobs, first, last, *refs):
    count = len(masks)
    sides = 1 + max(t for t, _ in jobs)
    flat_ref, lists_ref = refs[:2]
    targets = refs[2 : 2 + sides]
    packs = refs[2 + sides : 2 + sides + count]
    x_ref, p_ref, n_ref, acc_ref, todo_ref, x_sem, p_sem = refs[-7:]
    outs = refs[-7 - (2 if last else 1) : -7]
    flat = flat_ref[0]
    size, feats = targets[0].shape
    half = size // 2
    width = outs[0].shape[-1]
    tile = 128
    if not last:
        acc_ref = outs[0]
    hits = [listed(lists_ref, flat ^ t, flat ^ masks[k]).astype(jnp.int32) for t, k in jobs]
    for i, (t, k) in enumerate(jobs):
        todo_ref[0, i] = hits[i]
        todo_ref[1, i] = jnp.int32(t)
        todo_ref[2, i] = jnp.int32(k)
    moves = []
    for t in range(sides):
        need = sum(hit for hit, job in zip(hits, jobs) if job[0] == t)
        moves.append((need, pltpu.make_async_copy(targets[t], x_ref.at[t], x_sem.at[t])))
    for k in range(count):
        need = sum(hit for hit, job in zip(hits, jobs) if job[1] == k)
        moves.append((need, pltpu.make_async_copy(packs[k], p_ref.at[k], p_sem.at[k])))
    for i, (t, k) in enumerate(jobs):
        fresh = hits[i]
        for before, job in zip(hits[:i], jobs[:i]):
            if job[1] == k:
                fresh = fresh * (1 - before)
        todo_ref[3, i] = fresh
    for need, move in moves:
        pl.when(need > 0)(move.start)
    acc_ref[...] = jnp.zeros_like(acc_ref) if first else refs[2 + sides + count][...]

    def job(index, carry):
        active = todo_ref[0, index] > 0
        t = todo_ref[1, index]
        k = todo_ref[2, index]

        for side in range(sides):
            pl.when(active & (carry != t) & (t == side))(moves[side][1].wait)
        for pack in range(count):
            pl.when((todo_ref[3, index] > 0) & (k == pack))(moves[sides + pack][1].wait)

        @pl.when(jnp.logical_and(active, carry != t))
        def _():
            for i in range(size // 256):
                at = pl.ds(i * 256, 256)
                length, inv = norms(x_ref[t, at, :])
                n_ref[0, at, :] = length
                n_ref[1, at, :] = inv

        @pl.when(active)
        def _():
            parts = p_ref[k, half : half + 16, 0:half].astype(F32)
            inv_row = jnp.sum(parts, axis=0, keepdims=True)
            weights = p_ref[k, 0:half, feats : feats + 2 * width]
            for i in range(size // tile):
                at = pl.ds(i * tile, tile)
                c = dot(x_ref[t, at, :], p_ref[k, 0:half, 0:feats], ((1,), (1,)))
                hi, lo = halves(unit_kernel(c * n_ref[1, at, :] * inv_row))
                total = dot(hi, weights) + dot(lo, weights)
                acc_ref[t, at, :] += n_ref[0, at, :] * (total[:, 0:width] + total[:, width:])

        return jnp.where(active, t, carry)

    lax.fori_loop(0, len(jobs), job, -1)
    if last:
        outs[0][...] = acc_ref[0]
        outs[1][...] = acc_ref[1]


def basis_kernel(
    basis_hbm, w_hbm, first_hbm, perm_ref, turned_ref, part_ref, hot_ref, basis_ref, w_ref,
    first_ref, sem
):
    moves = []
    for k, (src, dst) in enumerate(
        ((basis_hbm, basis_ref), (w_hbm, w_ref), (first_hbm, first_ref))
    ):
        moves.append(pltpu.make_async_copy(src, dst, sem.at[k]))
        moves[k].start()
    size = basis_ref.shape[1]
    rank = basis_ref.shape[0]
    width = w_ref.shape[1]
    place = lax.rem(perm_ref[...], size)
    for i in range(size // 256):
        spot = lax.broadcasted_iota(jnp.int32, (256, size), 0) + i * 256
        hot_ref[i * 256 : (i + 1) * 256, :] = jnp.where(spot == place, 1.0, 0.0).astype(BF16)
    for move in moves:
        move.wait()
    hi, lo = halves(basis_ref[...])
    pair = jnp.concatenate([hi, lo], 0)
    hot = hot_ref[...]
    turned_ref[...] = dot(hot, pair, ((1,), (1,))).astype(BF16)
    moved = dot(pair, hot, ((1,), (1,))).astype(BF16)
    whi, wlo = halves(w_ref[...])
    y = dot(moved, jnp.concatenate([whi, wlo], 1))
    y = y[0:rank, 0:width] + y[0:rank, width:] + y[rank:, 0:width]
    part_ref[...] = three(first_ref[...], y, ((0,), (0,)))


def climb_kernel(flat_ref, part_ref, *refs):
    pairs, quads = refs[0:2], refs[2:6]
    keep_ref, send_ref, a_ref, b_ref = refs[6:]
    flat = flat_ref[0]
    half, quarter = pairs[0].shape[0], quads[0].shape[0]
    parity = flat % 2
    a_ref[...] = part_ref[...]
    total = None
    for k, ref in enumerate(pairs):
        at = pl.ds(pl.multiple_of((parity ^ k) * half, half), half)
        term = three(ref[...], a_ref[at, :], ((0,), (0,)))
        total = term if total is None else total + term
    b_ref[...] = total
    total = None
    for k, ref in enumerate(quads):
        at = pl.ds(pl.multiple_of(((flat % 4) ^ k) * quarter, quarter), quarter)
        term = three(ref[...], b_ref[at, :], ((0,), (0,)))
        total = term if total is None else total + term
    a_ref[...] = total
    keep_ref[...] = a_ref[pl.ds(pl.multiple_of(parity * half, half), half), :]
    send_ref[...] = a_ref[pl.ds(pl.multiple_of((1 - parity) * half, half), half), :]


def mate_sum_kernel(keep_ref, got_ref, pts_ref, out_ref):
    hi, lo = halves(keep_ref[...] + got_ref[...])
    half, width = keep_ref.shape
    out_ref[0:half, 0:width] = hi
    out_ref[0:half, width:] = lo
    out_ref[half:, :] = pts_ref[...]


def node_sum_kernel(*refs):
    ins, out_ref = refs[:-1], refs[-1]
    rows = (out_ref.shape[0] - ins[0].shape[0]) // (len(ins) - 1)
    half = ins[0].shape[0] - rows
    width = ins[0].shape[1] // 2
    total = None
    for k, ref in enumerate(ins):
        term = ref[0:half, 0:width].astype(F32) + ref[0:half, width:].astype(F32)
        total = term if total is None else total + term
        out_ref[half + k * rows : half + (k + 1) * rows, :] = ref[half:, :]
    hi, lo = halves(total)
    out_ref[0:half, 0:width] = hi
    out_ref[0:half, width:] = lo


def far_kernel(nodes, flat_ref, lists_ref, own_ref, mate_ref, b1_ref, *refs):
    pairs, quads = refs[0:2], refs[2:6]
    turned_ref, out_ref, pts_ref, w_ref, a_ref, b_ref = refs[6:]
    flat = flat_ref[0]
    rank = b1_ref.shape[1]
    half, quarter = pairs[0].shape[0], quads[0].shape[0]
    node, position, parity = flat // NODE, flat % NODE, flat % 2
    width = out_ref.shape[1]
    rows = rank // NODE
    for k, ref in enumerate((own_ref, mate_ref)):
        for m in range(nodes):
            at = (node ^ m) * rank + (parity ^ k) * half
            w_ref[pl.ds(pl.multiple_of(at, half), half), :] = ref[m, 0:half, :]
            for r in range(NODE // 2):
                at = (node ^ m) * rank + (position ^ (2 * r) ^ k) * rows
                low = half + r * rows
                pts_ref[pl.ds(pl.multiple_of(at, rows), rows), :] = ref[m, low : low + rows, :]
    feats = pts_ref.shape[1]
    left = pts_ref[pl.ds(pl.multiple_of(node * rank, rank), rank), :]
    length, inv = norms(left)
    up = jnp.zeros((rank, 2 * width), F32)
    for m in range(nodes):
        at = pl.ds(m * rank, rank)
        pts = pts_ref[at, :]
        wide = pts.astype(F32)
        shi, slo = halves(wide * wide)
        ones = jnp.ones((8, feats), BF16)
        row = dot(ones, shi, ((1,), (1,))) + dot(ones, slo, ((1,), (1,)))
        square = jnp.maximum(row[0:1, :], TINY)
        back = lax.rsqrt(square)
        c = dot(left, pts, ((1,), (1,)))
        scale = jnp.where(listed(lists_ref, node, m), 0.5, 0.0)
        hi, lo = halves(unit_kernel(c * inv * back) * (square * back * scale))
        up = up + dot(hi, w_ref[at, :]) + dot(lo, w_ref[at, :])
    up = length * (up[:, 0:width] + up[:, width:])
    for k, ref in enumerate(quads):
        at = pl.ds(pl.multiple_of(((flat % 4) ^ k) * quarter, quarter), quarter)
        a_ref[at, :] = three(ref[...], up)
    up = a_ref[...]
    for k, ref in enumerate(pairs):
        at = pl.ds(pl.multiple_of((parity ^ k) * half, half), half)
        b_ref[at, :] = three(ref[...], up)
    up = three(b1_ref[...], b_ref[...])
    hi, lo = halves(up)
    top = jnp.concatenate([hi, lo], 1)
    low = jnp.concatenate([hi, jnp.zeros_like(lo)], 1)
    far = dot(turned_ref[...], jnp.concatenate([top, low], 0))
    out_ref[...] = far[:, 0:width] + far[:, width:]


def join_kernel(a_ref, b_ref, c_ref, out_ref):
    out_ref[...] = (a_ref[...] + c_ref[...]) + b_ref[...]


def stack_kernel(*refs):
    for k, ref in enumerate(refs[:-1]):
        refs[-1][k] = ref[...]


def body(
    points, rhs, permutation, leaf_basis, climb_leaf, climb_pair, climb_quad, skel_points,
    near_lists, far_lists
):
    size, feats = points.shape
    width = rhs.shape[1]
    rank = climb_leaf.shape[1]
    nodes = lax.axis_size(AXES) // NODE
    flat = lax.axis_index(AXES).astype(jnp.int32).reshape(1)
    struct = jax.ShapeDtypeStruct

    quads = [climb_quad] + [across(climb_quad, k) for k in (1, 2, 3)]
    pairs = [climb_pair, across(climb_pair, 1)]

    mate_pts = across(points, 1)
    pack_shape = struct((size // 2 + 16, max(feats + 2 * width, size // 2)), BF16)
    pack_a, pack_b = call(
        pack_kernel, [pack_shape, pack_shape], 0, (points, rhs),
        [
            pltpu.VMEM((size, feats), BF16),
            pltpu.VMEM((size, width), F32),
            pltpu.SemaphoreType.DMA((4,)),
        ],
        flops=8 * 10**9,
        loose=2,
    )
    x_b, y_a = across(pack_b, 2), across(pack_a, 4)
    x_a, y_b = across(pack_a, 2), across(pack_b, 4)
    d_a = across(y_a, 2)
    d_b = across(x_b, 4)
    masks = [NODE * m for m in range(1, nodes)]

    block = 2 * size * size * (feats + 6 * width) * 4
    sums = struct((size, width), F32)

    def near(masks, jobs, packs, before=None, last=False):
        kernel = functools.partial(near_kernel, masks, jobs, before is None, last)
        before = () if before is None else (before,)
        sides = (points, mate_pts)[: 1 + max(t for t, _ in jobs)]
        loose = len(sides) + len(masks)
        return call(
            kernel, [sums, sums] if last else struct((2, size, width), F32), 2,
            (flat, near_lists, *sides, *packs, *before),
            [
                pltpu.VMEM((len(sides), size, feats), BF16),
                pltpu.VMEM((len(masks), *pack_shape.shape), BF16),
                pltpu.VMEM((2, size, 1), F32),
                pltpu.VMEM((2, size, width) if last else (8, 128), F32),
                pltpu.SMEM((4, len(jobs)), jnp.int32),
                pltpu.SemaphoreType.DMA((len(sides),)),
                pltpu.SemaphoreType.DMA((len(masks),)),
            ],
            flops=block * len(jobs) // 2,
            loose=loose,
        )

    turned, part = call(
        basis_kernel,
        [struct((size, 2 * rank), BF16), struct((rank, width), F32)],
        0,
        (leaf_basis, rhs, climb_leaf, permutation.reshape(1, size)),
        [
            pltpu.VMEM((size, size), BF16),
            pltpu.VMEM((rank, size), F32),
            pltpu.VMEM((size, width), F32),
            pltpu.VMEM((rank, rank), F32),
            pltpu.SemaphoreType.DMA((3,)),
        ],
        loose=3,
        flops=2 * size * size * rank * 6,
    )
    strip = struct((rank // 2, width), F32)
    keep, send = call(
        climb_kernel, [strip, strip], 1, (flat, part, *pairs, *quads),
        [pltpu.VMEM((rank, width), F32), pltpu.VMEM((rank, width), F32)],
        flops=2 * rank * rank * width * 12,
    )
    rows = rank // 2 + skel_points.shape[0]
    strip = call(
        mate_sum_kernel, struct((rows, 2 * width), BF16), 0,
        (keep, across(send, 1), skel_points),
    )
    strips = [strip] + [across(strip, k) for k in (2, 4, 6)]
    rows = rank // 2 + 4 * skel_points.shape[0]
    value = call(node_sum_kernel, struct((rows, 2 * width), BF16), 0, tuple(strips))
    others = [across(value, m) for m in masks]
    every = call(stack_kernel, struct((nodes, *value.shape), BF16), 0, (value, *others))
    every_mate = across(every, 1)

    own = (pack_a, pack_b)
    total = near((0, 0), ((0, 0), (0, 1), (1, 0), (1, 1)), own)
    jobs = [(t, k) for t in range(2) for k in range(4)]
    total = near((2, 2, 4, 4), jobs, (x_a, x_b, y_a, y_b), total)
    jobs = ((0, 0), (0, 1), (1, 0), (1, 1))
    mine, other = near((6, 6), jobs, (d_a, d_b), total, True)
    far = call(
        functools.partial(far_kernel, nodes),
        sums,
        2,
        (
            flat, far_lists, every, every_mate, climb_leaf, *pairs, *quads, turned
        ),
        [
            pltpu.VMEM((nodes * rank, feats), BF16),
            pltpu.VMEM((nodes * rank, 2 * width), BF16),
            pltpu.VMEM((rank, width), F32),
            pltpu.VMEM((rank, width), F32),
        ],
        flops=2 * rank * rank * width * 60,
    )
    return call(join_kernel, sums, 0, (mine, across(other, 1), far))


def solution(mesh):
    split = P(AXES, None)

    return jax.shard_map(
        body,
        mesh=mesh,
        in_specs=(split, split, P(AXES), split, split, split, split, split, P(), P()),
        out_specs=split,
        check_vma=False,
    )
```
